256 devices in a mesh: ep: 16 (over y, x), fsdp: 16 (over z, core).
Axes of the slice: x: 4, y: 4, z: 8, core: 2. Of those that a mesh axis runs over, the one named last changes fastest.
Arguments:
- w_gate: float32 [64, 2048, 1024], P('ep', 'fsdp'), may hold values from -0.1875 to 0.1875
- avg_gate: bfloat16 [64, 2048, 1024], P('ep', 'fsdp'), may hold values from -0.0625 to 0.0625
- w_up: float32 [64, 2048, 1024], P('ep', 'fsdp'), may hold values from -0.1875 to 0.1875
- avg_up: bfloat16 [64, 2048, 1024], P('ep', 'fsdp'), may hold values from -0.0625 to 0.0625
- w_down: float32 [64, 1024, 2048], P('ep', None, 'fsdp'), may hold values from -0.25 to 0.25
- avg_down: bfloat16 [64, 1024, 2048], P('ep', None, 'fsdp'), may hold values from -0.09375 to 0.09375
- router_weight: float32 [2048, 64], P('fsdp', 'ep'), may hold values from -0.125 to 0.125
- router_gain: float32 [2048], P('fsdp'), may hold values from 0.25 to 1.75
Outputs:
- serve_gate: bfloat16 [64, 2048, 1024], P('ep', None, 'fsdp')
- serve_up: bfloat16 [64, 2048, 1024], P('ep', None, 'fsdp')
- serve_down: bfloat16 [64, 1024, 2048], P('ep', 'fsdp')
- scale_gate: float32 [64, 1024], P('ep', 'fsdp')
- scale_up: float32 [64, 1024], P('ep', 'fsdp')
- scale_down: float32 [64, 1024], P('ep', 'fsdp')
- serve_router: bfloat16 [2048, 64], replicated
The draws below stay inside these ranges and needn't reach their ends.
All inputs are finite; a program needn't handle non-finite values.
Results may differ from the reference program's by a relative error of at most 0.001.
Values may be sent and summed in bfloat16 or wider, within the bound.
A program may use at most 64 MiB of HBM per device.

```python
import jax
import jax.numpy as jnp
from jax import lax

EXPERTS = 64
D_MODEL = 2048
D_EXPERT = 1024


def with_spikes(result, stream_key, source, target, blocks, factor):
    owner, partner = [(jnp.arange(result.shape[axis_at]) // (result.shape[axis_at] // blocks)).reshape([-1 if axis == axis_at else 1 for axis in range(result.ndim)]) for axis_at in (source, target)]
    chosen = jax.random.permutation(stream_key, blocks)[partner]
    strong = (owner == chosen) | (owner == (partner + blocks // 2) % blocks)
    return jnp.where(strong, factor * result, result)


def levels(rng, shape, split, least, top_value):
    gain, own = 1.0, jax.random.fold_in(rng, 6)
    for position, shards_of in split:
        steps = jnp.exp(jax.random.uniform(jax.random.fold_in(own, position), (shards_of,), jnp.float32, least / len(split), top_value / len(split)))
        gain = gain * jnp.repeat(steps, shape[position] // shards_of).reshape([-1 if axis == position else 1 for axis in range(len(shape))])
    return gain


def centred(rng, dims, width, bound, cuts=(), kind=jnp.bfloat16):
    drawn = jax.random.normal(rng, dims, jnp.float32) * width
    if len(cuts) > 0:
        drawn = levels(rng, dims, cuts, -0.22, 0.18) * drawn
    return jnp.clip(drawn, min=-bound, max=bound).astype(kind)


def gaussian_with(stream_key, shape, spread, reach, split, heavy, dtype=jnp.bfloat16):
    values = spread * jax.random.normal(stream_key, shape, jnp.float32)
    if split:
        values = values * levels(stream_key, shape, split, -0.22, 0.18)
    return jnp.clip(with_spikes(values, jax.random.fold_in(stream_key, 3), *heavy), -reach, reach).astype(dtype)


def setup_inputs(seed: int = 0) -> dict:
    splits = jax.random.split(jax.random.key(seed), 9)
    w_gate = gaussian_with(splits[0], (EXPERTS, D_MODEL, D_EXPERT), D_MODEL ** -0.5, 0.1875, ((0, 16), (1, 16)), (1, 2, 16, 2.0), jnp.float32)
    avg_gate = centred(splits[1], (EXPERTS, D_MODEL, D_EXPERT), (D_MODEL * 4) ** -0.5, 0.0625, ((0, 16), (1, 16)))
    w_up = gaussian_with(splits[2], (EXPERTS, D_MODEL, D_EXPERT), D_MODEL ** -0.5, 0.1875, ((0, 16), (1, 16)), (1, 2, 16, 2.0), jnp.float32)
    avg_up = centred(splits[3], (EXPERTS, D_MODEL, D_EXPERT), (D_MODEL * 4) ** -0.5, 0.0625, ((0, 16), (1, 16)))
    w_down = gaussian_with(splits[4], (EXPERTS, D_EXPERT, D_MODEL), D_EXPERT ** -0.5, 0.25, ((0, 16), (2, 16)), (2, 1, 16, 2.0), jnp.float32)
    avg_down = centred(splits[5], (EXPERTS, D_EXPERT, D_MODEL), (D_EXPERT * 4) ** -0.5, 0.09375, ((0, 16), (2, 16)))
    router_weight = centred(splits[6], (D_MODEL, EXPERTS), D_MODEL ** -0.5, 0.125, ((0, 16), (1, 16)), jnp.float32)
    router_gain = jnp.clip(1.0 + 0.15 * jax.random.normal(splits[7], (D_MODEL,), jnp.float32), 0.25, 1.75)
    return {"w_gate": w_gate, "avg_gate": avg_gate, "w_up": w_up, "avg_up": avg_up, "w_down": w_down, "avg_down": avg_down, "router_weight": router_weight, "router_gain": router_gain}


def reference(w_gate, avg_gate, w_up, avg_up, w_down, avg_down, router_weight, router_gain):
    fresh_gate = w_gate + avg_gate.astype(jnp.float32)
    fresh_up = w_up + avg_up.astype(jnp.float32)
    fresh_down = w_down + avg_down.astype(jnp.float32)
    scale_gate = jnp.sqrt(lax.optimization_barrier(jnp.sum(fresh_gate * fresh_gate, axis=1)))
    serve_gate = (fresh_gate / jnp.expand_dims(scale_gate, 1)).astype(jnp.bfloat16)
    scale_up = jnp.sqrt(lax.optimization_barrier(jnp.sum(fresh_up * fresh_up, axis=1)))
    serve_up = (fresh_up / jnp.expand_dims(scale_up, 1)).astype(jnp.bfloat16)
    scale_down = jnp.sqrt(lax.optimization_barrier(jnp.sum(fresh_down * fresh_down, axis=2)))
    serve_down = (fresh_down / jnp.expand_dims(scale_down, 2)).astype(jnp.bfloat16)
    serve_router = (router_weight * router_gain[:, None]).astype(jnp.bfloat16)
    return (serve_gate, serve_up, serve_down, scale_gate, scale_up, scale_down, serve_router)
```

```python
import jax
import jax.numpy as jnp
from jax import lax
from jax.experimental import pallas as pl
from jax.experimental.pallas import tpu as pltpu
from jax.sharding import PartitionSpec as P

MESH = pl.DeviceIdType.MESH
RING = 8
PEERS = 2 * RING
EACH = 4
UNITS = 3 * EACH
LANES = 128
HALF = 64
FAR_FIRST = (4, 3, -3, 2, -2, 1, -1)


def others(me):
    chip, core = me // 2, me % 2
    found = [2 * chip + 1 - core]
    for step in FAR_FIRST:
        there = lax.rem(chip + step + RING, RING)
        found += [2 * there + core, 2 * there + 1 - core]
    return found


def block(i):
    return pl.ds(pl.multiple_of(i * LANES, LANES), LANES)


def wait_for(ref, sem):
    pltpu.make_async_copy(ref, ref, sem).wait()


def exchange(
    w_gate, avg_gate, w_up, avg_up, w_down, avg_down, router_weight, router_gain,
    out, own_total, router,
    fresh, change, raw, raw_change, weight, gain,
    even, odd, parts, got, total, totals, inverse, ready, rows, columns,
    load_sem, part_send, part_recv, total_send, total_recv,
    send, recv, row_send, row_recv, column_send, column_recv,
):
    me, group = lax.axis_index("fsdp"), lax.axis_index("ep")
    barrier = pltpu.get_barrier_semaphore()

    def greet(i, _):
        pl.semaphore_signal(barrier, inc=1, device_id={"fsdp": lax.rem(me + i, PEERS)}, device_id_type=MESH)
        pl.semaphore_signal(barrier, inc=1, device_id={"ep": lax.rem(group + i, PEERS)}, device_id_type=MESH)
        return 0

    lax.fori_loop(1, PEERS, greet, 0)
    loads = []
    for w, avg, at in ((w_gate, avg_gate, 0), (w_up, avg_up, EACH)):
        for e in range(EACH):
            loads.append((w.at[e], fresh.at[at + e]))
            loads.append((avg.at[e], change.at[at + e]))
    for e in range(EACH):
        loads.append((w_down.at[e], raw.at[e]))
        loads.append((avg_down.at[e], raw_change.at[e]))
    loads += [(router_weight, weight), (router_gain, gain)]
    loads = [pltpu.make_async_copy(a, b, load_sem.at[i]) for i, (a, b) in enumerate(loads)]
    for copy in loads:
        copy.start()

    even[6:8, :] = jnp.zeros((2, even.shape[1]), jnp.float32)
    odd[6:8, :] = jnp.zeros((2, odd.shape[1]), jnp.float32)

    for u in range(UNITS):
        loads[2 * u].wait()
        loads[2 * u + 1].wait()
        sums, row = (even, odd)[u % 2], u // 2
        if u < 2 * EACH:

            def add_up(i, acc):
                at = pl.ds(pl.multiple_of(i * 16, 16), 16)
                x = fresh[u, at, :] + change[u, at, :].astype(jnp.float32)
                fresh[u, at, :] = x
                x = x * x
                return acc + x[:8] + x[8:]

            acc = lax.fori_loop(0, 8, add_up, jnp.zeros((8, 1024), jnp.float32))
            sums[row : row + 1, :] = jnp.sum(acc, axis=0, keepdims=True)
        else:
            e = u - 2 * EACH

            def add_across(b, _):
                x = raw[e, block(b), :] + raw_change[e, block(b), :].astype(jnp.float32)
                x = x.T
                fresh[u, :, block(b)] = x
                sums[row : row + 1, block(b)] = jnp.sum(x * x, axis=0, keepdims=True)
                return 0

            lax.fori_loop(0, 8, add_across, 0)
    loads[-2].wait()
    loads[-1].wait()
    rows[:, block(me)] = (weight[...] * gain[...]).astype(jnp.bfloat16)

    low = lax.broadcasted_iota(jnp.int32, (8, LANES), 1) < HALF
    first = jnp.concatenate([even[0:1, LANES * z : LANES * (z + 1)] for z in range(RING)], axis=0)
    for z in range(RING):
        a, b = even[:, LANES * z : LANES * (z + 1)], odd[:, LANES * z : LANES * (z + 1)]
        parts[2 * z, 0:8, :] = jnp.where(low, a, pltpu.roll(b, HALF, 1))
        parts[2 * z + 1, 0:8, :] = jnp.where(low, pltpu.roll(a, HALF, 1), b)
        parts[2 * z, 8:16, :] = first
        parts[2 * z + 1, 8:16, :] = first
    got[me] = parts[me]

    pl.semaphore_wait(barrier, 2 * (PEERS - 1))
    peers = others(me)

    def push(src, dst, send_sem, recv_sem, where):
        pltpu.make_async_remote_copy(
            src_ref=src, dst_ref=dst, send_sem=send_sem, recv_sem=recv_sem, device_id=where, device_id_type=MESH
        ).start()

    for d in peers:
        push(parts.at[d], got.at[me], part_send, part_recv, {"fsdp": d})
    for d in peers:
        push(rows.at[:, block(me)], rows.at[:, block(me)], row_send, row_recv, {"fsdp": d})

    def normalise(u):
        for z in range(RING):
            x = fresh[u, :, LANES * z : LANES * (z + 1)] * inverse[u, z : z + 1, :]
            x = x.T.astype(jnp.bfloat16)
            ready[u, 2 * z] = x[:HALF]
            ready[u, 2 * z + 1] = x[HALF:]
        out[u, :, block(me)] = ready[u, me]

    def spread(u):
        for d in peers:
            push(ready.at[u, d], out.at[u, :, block(me)], send.at[u], recv.at[u], {"fsdp": d})

    wait_for(got.at[pl.ds(0, PEERS - 1)], part_recv)
    summed = got[0]
    for d in range(1, PEERS):
        summed = summed + got[d]
    total[...] = summed[0:8]
    totals[me] = summed[0:8]
    own_total[...] = summed[0:8]
    inverse[0] = 1.0 / jnp.sqrt(summed[8:16])
    for d in peers:
        push(total, totals.at[me], total_send, total_recv, {"fsdp": d})
    normalise(0)
    spread(0)

    wait_for(rows.at[:, pl.ds(0, LANES * (PEERS - 1))], row_recv)
    columns[group] = rows[...]

    def to_group(i, _):
        push(rows, columns.at[group], column_send, column_recv, {"ep": lax.rem(group + i, PEERS)})
        return 0

    lax.fori_loop(1, PEERS, to_group, 0)

    wait_for(totals.at[pl.ds(0, PEERS - 1)], total_recv)
    for z in range(RING):
        a, b = 1.0 / jnp.sqrt(totals[2 * z]), 1.0 / jnp.sqrt(totals[2 * z + 1])
        c, d = jnp.where(low, a, pltpu.roll(b, HALF, 1)), jnp.where(low, pltpu.roll(a, HALF, 1), b)
        for r in range(UNITS // 2):
            inverse[2 * r, z : z + 1, :] = c[r : r + 1]
            inverse[2 * r + 1, z : z + 1, :] = d[r : r + 1]

    def step(u, _):
        normalise(u)
        spread(u)
        return 0

    lax.fori_loop(1, UNITS, step, 0)

    wait_for(columns.at[pl.ds(0, PEERS - 1)], column_recv)
    for p in range(PEERS):
        router[4 * p : 4 * p + 4, :] = columns[p]

    def arrive(u, _):
        wait_for(out.at[u, :, pl.ds(0, LANES * (PEERS - 1))], recv.at[u])
        wait_for(ready.at[u, pl.ds(0, PEERS - 1)], send.at[u])
        return 0

    lax.fori_loop(0, UNITS, arrive, 0)
    wait_for(parts.at[pl.ds(0, PEERS - 1)], part_send)
    wait_for(totals.at[pl.ds(0, PEERS - 1)], total_send)
    wait_for(rows.at[:, pl.ds(0, LANES * (PEERS - 1))], row_send)
    wait_for(columns.at[pl.ds(0, PEERS - 1)], column_send)


def settle(out, own_total, router, gate, up, down, scale_gate, scale_up, scale_down, serve_router, sem):
    copies = [
        pltpu.make_async_copy(out.at[pl.ds(EACH * i, EACH)], to, sem.at[i]) for i, to in enumerate((gate, up, down))
    ]
    copies.append(pltpu.make_async_copy(router, serve_router, sem.at[3]))
    for copy in copies:
        copy.start()
    for i, scale in enumerate((scale_gate, scale_up, scale_down)):
        for e in range(EACH):
            r, h = divmod(EACH * i + e, 2)
            scale[e : e + 1, :] = jnp.sqrt(own_total[r : r + 1, HALF * h : HALF * (h + 1)])
    for copy in copies:
        copy.wait()


def on_device(w_gate, avg_gate, w_up, avg_up, w_down, avg_down, router_weight, router_gain):
    f32, bf16 = jnp.float32, jnp.bfloat16
    hbm, vmem = pl.BlockSpec(memory_space=pltpu.HBM), pl.BlockSpec(memory_space=pltpu.VMEM)
    dma = pltpu.SemaphoreType.DMA
    held = pl.pallas_call(
        exchange,
        out_shape=(
            pltpu.VMEM((UNITS, HALF, 2048), bf16),
            pltpu.VMEM((8, LANES), f32),
            pltpu.VMEM((HALF, 2048), bf16),
        ),
        in_specs=[hbm] * 8,
        out_specs=(vmem,) * 3,
        scratch_shapes=[
            pltpu.VMEM((UNITS, LANES, 1024), f32),
            pltpu.VMEM((2 * EACH, LANES, 1024), bf16),
            pltpu.VMEM((EACH, 1024, LANES), f32),
            pltpu.VMEM((EACH, 1024, LANES), bf16),
            pltpu.VMEM((4, LANES), f32),
            pltpu.VMEM((1, LANES), f32),
            pltpu.VMEM((8, 1024), f32),
            pltpu.VMEM((8, 1024), f32),
            pltpu.VMEM((PEERS, 16, LANES), f32),
            pltpu.VMEM((PEERS, 16, LANES), f32),
            pltpu.VMEM((8, LANES), f32),
            pltpu.VMEM((PEERS, 8, LANES), f32),
            pltpu.VMEM((UNITS, RING, LANES), f32),
            pltpu.VMEM((UNITS, PEERS, HALF, LANES), bf16),
            pltpu.VMEM((4, 2048), bf16),
            pltpu.VMEM((PEERS, 4, 2048), bf16),
            dma((2 * UNITS + 2,)),
            dma(()), dma(()), dma(()), dma(()),
            dma((UNITS,)), dma((UNITS,)),
            dma(()), dma(()), dma(()), dma(()),
        ],
        compiler_params=pltpu.CompilerParams(
            collective_id=0, has_side_effects=True, vmem_limit_bytes=60 << 20
        ),
        name="exchange",
    )(w_gate, avg_gate, w_up, avg_up, w_down, avg_down, router_weight.T, router_gain[None, :])
    served = jax.ShapeDtypeStruct((EACH, HALF, 2048), bf16)
    scale = jax.ShapeDtypeStruct((EACH, HALF), f32)
    gate, up, down, scale_gate, scale_up, scale_down, router = pl.pallas_call(
        settle,
        out_shape=(served, served, served, scale, scale, scale, jax.ShapeDtypeStruct((HALF, 2048), bf16)),
        in_specs=[vmem] * 3,
        out_specs=(hbm, hbm, hbm, vmem, vmem, vmem, hbm),
        scratch_shapes=[dma((4,))],
        compiler_params=pltpu.CompilerParams(vmem_limit_bytes=8 << 20),
        name="settle",
    )(*held)
    turned = (0, 2, 1)
    return (
        gate.transpose(turned), up.transpose(turned), down, scale_gate, scale_up, scale_down, router.T
    )


def solution(mesh):
    placed = (
        P("ep", "fsdp", None),
        P("ep", "fsdp", None),
        P("ep", "fsdp", None),
        P("ep", "fsdp", None),
        P("ep", None, "fsdp"),
        P("ep", None, "fsdp"),
        P("fsdp", "ep"),
        P("fsdp"),
    )
    return jax.shard_map(
        on_device,
        mesh=mesh,
        in_specs=placed,
        out_specs=(
            P("ep", None, "fsdp"),
            P("ep", None, "fsdp"),
            P("ep", "fsdp", None),
            P("ep", "fsdp"),
            P("ep", "fsdp"),
            P("ep", "fsdp"),
            P(),
        ),
        check_vma=False,
    )
```

```python
import jax
import jax.numpy as jnp
from jax import lax
from jax.experimental import pallas as pl
from jax.experimental.pallas import tpu as pltpu
from jax.sharding import PartitionSpec as P

MESH = pl.DeviceIdType.MESH
RING = 8
PEERS = 2 * RING
AHEAD = (2, 1)
SHIFT = 6
EACH = 4
UNITS = 3 * EACH
LANES = 128
HALF = 64
IN_ORDER = tuple(range(2 * EACH, UNITS)) + tuple(range(2 * EACH))
FAR_FIRST = (4, 3, -3, 2, -2, 1, -1)


def others(me):
    chip, core = me // 2, me % 2
    found = []
    for step in FAR_FIRST:
        there = lax.rem(chip + step + RING, RING)
        found += [2 * there + core, 2 * there + 1 - core]
    return found + [2 * chip + 1 - core]


def block(i):
    return pl.ds(pl.multiple_of(i * LANES, LANES), LANES)


def wait_for(ref, sem):
    pltpu.make_async_copy(ref, ref, sem).wait()


def exchange(
    w_gate, avg_gate, w_up, avg_up, w_down, avg_down, router_weight, router_gain,
    out, own_total, router,
    fresh, change, raw, raw_change, weight, gain,
    even, odd, parts, got, total, totals, inverse, ready, rows, columns,
    load_sem, part_send, part_recv, total_send, total_recv,
    send, recv, row_send, row_recv, column_send, column_recv,
):
    me, group = lax.axis_index("fsdp"), lax.axis_index("ep")
    barrier = pltpu.get_barrier_semaphore()

    peers = others(me)

    def greet(where):
        pl.semaphore_signal(barrier, inc=1, device_id=where, device_id_type=MESH)

    for d in peers:
        greet({"fsdp": d})
    loads = []
    for w, avg, at in ((w_gate, avg_gate, 0), (w_up, avg_up, EACH)):
        for e in range(EACH):
            loads.append((w.at[e], fresh.at[at + e]))
            loads.append((avg.at[e], change.at[at + e]))
    for e in range(EACH):
        loads.append((w_down.at[e], raw.at[e]))
        loads.append((avg_down.at[e], raw_change.at[e]))
    loads += [(router_weight, weight), (router_gain, gain)]
    loads = [pltpu.make_async_copy(a, b, load_sem.at[i]) for i, (a, b) in enumerate(loads)]
    for copy in loads[-2:] + [loads[2 * u + i] for u in IN_ORDER for i in range(2)]:
        copy.start()
    for i in range(1, PEERS):
        greet({"ep": lax.rem(group + i, PEERS)})

    even[6:8, :] = jnp.zeros((2, even.shape[1]), jnp.float32)
    odd[6:8, :] = jnp.zeros((2, odd.shape[1]), jnp.float32)

    for u in IN_ORDER:
        loads[2 * u].wait()
        loads[2 * u + 1].wait()
        sums, row = (even, odd)[u % 2], u // 2
        if u < 2 * EACH:

            def add_up(i, acc):
                at = pl.ds(pl.multiple_of(i * 16, 16), 16)
                x = fresh[u, at, :] + change[u, at, :].astype(jnp.float32)
                fresh[u, at, :] = x
                x = x * x
                return acc + x[:8] + x[8:]

            acc = lax.fori_loop(0, 8, add_up, jnp.zeros((8, 1024), jnp.float32), unroll=True)
            sums[row : row + 1, :] = jnp.sum(acc, axis=0, keepdims=True)
        else:
            e = u - 2 * EACH

            def add_across(b, _):
                x = raw[e, block(b), :] + raw_change[e, block(b), :].astype(jnp.float32)
                x = x.T
                fresh[u, :, block(b)] = x
                sums[row : row + 1, block(b)] = jnp.sum(x * x, axis=0, keepdims=True)
                return 0

            lax.fori_loop(0, 8, add_across, 0, unroll=True)
    loads[-2].wait()
    loads[-1].wait()
    rows[:, block(me)] = (weight[...] * gain[...]).astype(jnp.bfloat16)

    low = lax.broadcasted_iota(jnp.int32, (8, LANES), 1) < HALF
    first = jnp.concatenate([even[0:1, LANES * z : LANES * (z + 1)] for z in range(RING)], axis=0)
    for z in range(RING):
        a, b = even[:, LANES * z : LANES * (z + 1)], odd[:, LANES * z : LANES * (z + 1)]
        parts[2 * z, 0:8, :] = jnp.where(low, a, pltpu.roll(b, HALF, 1))
        parts[2 * z + 1, 0:8, :] = jnp.where(low, pltpu.roll(a, HALF, 1), b)
        parts[2 * z, 8:16, :] = first
        parts[2 * z + 1, 8:16, :] = first
    got[me] = parts[me]

    pl.semaphore_wait(barrier, 2 * (PEERS - 1))

    def push(src, dst, send_sem, recv_sem, where):
        pltpu.make_async_remote_copy(
            src_ref=src, dst_ref=dst, send_sem=send_sem, recv_sem=recv_sem, device_id=where, device_id_type=MESH
        ).start()

    for d in peers:
        push(parts.at[d], got.at[me], part_send, part_recv, {"fsdp": d})
    for d in peers:
        push(rows.at[:, block(me)], rows.at[:, block(me)], row_send, row_recv, {"fsdp": d})

    def normalise(u):
        for z in range(RING):
            x = fresh[u, :, LANES * z : LANES * (z + 1)] * inverse[u, z : z + 1, :]
            x = x.T.astype(jnp.bfloat16)
            ready[u, 2 * z] = x[:HALF]
            ready[u, 2 * z + 1] = x[HALF:]
        out[u, :, block(me)] = ready[u, me]

    def to_peer(u, d):
        push(ready.at[u, d], out.at[u, :, block(me)], send.at[u], recv.at[u], {"fsdp": d})

    def spread(u):
        for d in peers:
            to_peer(u, d)

    wait_for(got.at[pl.ds(0, PEERS - 1)], part_recv)
    summed = got[0]
    for d in range(1, PEERS):
        summed = summed + got[d]
    total[...] = summed[0:8]
    totals[me] = summed[0:8]
    own_total[...] = summed[0:8]
    inverse[0] = 1.0 / jnp.sqrt(summed[8:16])
    for d in peers:
        push(total, totals.at[me], total_send, total_recv, {"fsdp": d})
    normalise(0)
    spread(0)

    wait_for(rows.at[:, pl.ds(0, LANES * (PEERS - 1))], row_recv)
    columns[group] = rows[...]

    def to_group(i, _):
        push(rows, columns.at[group], column_send, column_recv, {"ep": lax.rem(group + i, PEERS)})
        return 0

    lax.fori_loop(1, PEERS, to_group, 0)

    wait_for(totals.at[pl.ds(0, PEERS - 1)], total_recv)
    for z in range(RING):
        a, b = 1.0 / jnp.sqrt(totals[2 * z]), 1.0 / jnp.sqrt(totals[2 * z + 1])
        c, d = jnp.where(low, a, pltpu.roll(b, HALF, 1)), jnp.where(low, pltpu.roll(a, HALF, 1), b)
        for r in range(UNITS // 2):
            inverse[2 * r, z : z + 1, :] = c[r : r + 1]
            inverse[2 * r + 1, z : z + 1, :] = d[r : r + 1]

    def step(u, _):
        normalise(u)
        spread(u)
        return 0

    def lead(d):
        return sum((d < 2 * chips).astype(jnp.int32) for chips in AHEAD)

    def spread_ahead(u, opens):
        for d in peers:
            if opens:
                to_peer(u, d)
                for i in range(1, len(AHEAD) + 1):
                    pl.when(lead(d) >= i)(lambda d=d, i=i: to_peer(u + i, d))
            else:
                unit = u + lead(d)
                pl.when(unit < UNITS)(lambda unit=unit, d=d: to_peer(unit, d))

    def step_ahead(u, _):
        pl.when(u + len(AHEAD) < UNITS)(lambda: normalise(u + len(AHEAD)))
        spread_ahead(u, False)
        return 0

    lax.fori_loop(1, SHIFT, step, 0)
    for i in range(len(AHEAD) + 1):
        normalise(SHIFT + i)
    spread_ahead(SHIFT, True)
    lax.fori_loop(SHIFT + 1, UNITS, step_ahead, 0)

    wait_for(columns.at[pl.ds(0, PEERS - 1)], column_recv)
    for p in range(PEERS):
        router[4 * p : 4 * p + 4, :] = columns[p]

    def arrive(u, _):
        wait_for(out.at[u, :, pl.ds(0, LANES * (PEERS - 1))], recv.at[u])
        wait_for(ready.at[u, pl.ds(0, PEERS - 1)], send.at[u])
        return 0

    lax.fori_loop(0, UNITS, arrive, 0)
    wait_for(parts.at[pl.ds(0, PEERS - 1)], part_send)
    wait_for(totals.at[pl.ds(0, PEERS - 1)], total_send)
    wait_for(rows.at[:, pl.ds(0, LANES * (PEERS - 1))], row_send)
    wait_for(columns.at[pl.ds(0, PEERS - 1)], column_send)


def settle(
    out, own_total, router, gate, up, down, scale_gate, scale_up, scale_down, serve_router, a, b, c, sem
):
    copies = [(out.at[pl.ds(EACH * i, EACH)], to) for i, to in enumerate((gate, up, down))]
    copies.append((router, serve_router))
    copies += [(a, scale_gate), (b, scale_up), (c, scale_down)]
    copies = [pltpu.make_async_copy(x, y, sem.at[i]) for i, (x, y) in enumerate(copies)]
    for copy in copies[:4]:
        copy.start()
    for i, scale in enumerate((a, b, c)):
        for e in range(EACH):
            r, h = divmod(EACH * i + e, 2)
            scale[e : e + 1, :] = jnp.sqrt(own_total[r : r + 1, HALF * h : HALF * (h + 1)])
    for copy in copies[4:]:
        copy.start()
    for copy in copies:
        copy.wait()


def on_device(w_gate, avg_gate, w_up, avg_up, w_down, avg_down, router_weight, router_gain):
    f32, bf16 = jnp.float32, jnp.bfloat16
    hbm, vmem = pl.BlockSpec(memory_space=pltpu.HBM), pl.BlockSpec(memory_space=pltpu.VMEM)
    dma = pltpu.SemaphoreType.DMA
    held = pl.pallas_call(
        exchange,
        out_shape=(
            pltpu.VMEM((UNITS, HALF, 2048), bf16),
            pltpu.VMEM((8, LANES), f32),
            pltpu.VMEM((HALF, 2048), bf16),
        ),
        in_specs=[hbm] * 8,
        out_specs=(vmem,) * 3,
        scratch_shapes=[
            pltpu.VMEM((UNITS, LANES, 1024), f32),
            pltpu.VMEM((2 * EACH, LANES, 1024), bf16),
            pltpu.VMEM((EACH, 1024, LANES), f32),
            pltpu.VMEM((EACH, 1024, LANES), bf16),
            pltpu.VMEM((4, LANES), f32),
            pltpu.VMEM((1, LANES), f32),
            pltpu.VMEM((8, 1024), f32),
            pltpu.VMEM((8, 1024), f32),
            pltpu.VMEM((PEERS, 16, LANES), f32),
            pltpu.VMEM((PEERS, 16, LANES), f32),
            pltpu.VMEM((8, LANES), f32),
            pltpu.VMEM((PEERS, 8, LANES), f32),
            pltpu.VMEM((UNITS, RING, LANES), f32),
            pltpu.VMEM((UNITS, PEERS, HALF, LANES), bf16),
            pltpu.VMEM((4, 2048), bf16),
            pltpu.VMEM((PEERS, 4, 2048), bf16),
            dma((2 * UNITS + 2,)),
            dma(()), dma(()), dma(()), dma(()),
            dma((UNITS,)), dma((UNITS,)),
            dma(()), dma(()), dma(()), dma(()),
        ],
        compiler_params=pltpu.CompilerParams(
            collective_id=0, has_side_effects=True, vmem_limit_bytes=60 << 20
        ),
        name="exchange",
    )(w_gate, avg_gate, w_up, avg_up, w_down, avg_down, router_weight.T, router_gain[None, :])
    served = jax.ShapeDtypeStruct((EACH, HALF, 2048), bf16)
    scale = jax.ShapeDtypeStruct((EACH, HALF), f32)
    gate, up, down, scale_gate, scale_up, scale_down, router = pl.pallas_call(
        settle,
        out_shape=(served, served, served, scale, scale, scale, jax.ShapeDtypeStruct((HALF, 2048), bf16)),
        in_specs=[vmem] * 3,
        out_specs=(hbm,) * 7,
        scratch_shapes=[pltpu.VMEM((EACH, HALF), f32)] * 3 + [dma((7,))],
        compiler_params=pltpu.CompilerParams(vmem_limit_bytes=8 << 20),
        name="settle",
    )(*held)
    turned = (0, 2, 1)
    return (
        gate.transpose(turned), up.transpose(turned), down, scale_gate, scale_up, scale_down, router.T
    )


def solution(mesh):
    placed = (
        P("ep", "fsdp", None),
        P("ep", "fsdp", None),
        P("ep", "fsdp", None),
        P("ep", "fsdp", None),
        P("ep", None, "fsdp"),
        P("ep", None, "fsdp"),
        P("fsdp", "ep"),
        P("fsdp"),
    )
    return jax.shard_map(
        on_device,
        mesh=mesh,
        in_specs=placed,
        out_specs=(
            P("ep", None, "fsdp"),
            P("ep", None, "fsdp"),
            P("ep", "fsdp", None),
            P("ep", "fsdp"),
            P("ep", "fsdp"),
            P("ep", "fsdp"),
            P(),
        ),
        check_vma=False,
    )
```

```python
import jax
import jax.numpy as jnp
from jax import lax
from jax.experimental import pallas as pl
from jax.experimental.pallas import tpu as pltpu
from jax.sharding import PartitionSpec as P

MESH = pl.DeviceIdType.MESH
RING = 8
PEERS = 2 * RING
AHEAD = (2, 1)
SHIFT = 9
EACH = 4
UNITS = 3 * EACH
LANES = 128
HALF = 64
PAIRS = UNITS // 2
SOON = 3
IN_ORDER = tuple(range(2 * SOON)) + tuple(range(2 * EACH, UNITS)) + tuple(range(2 * SOON, 2 * EACH))
BEFORE_BARRIER = 8
FAR_FIRST = (4, 3, -3, 2, -2, 1, -1)


def others(me):
    chip, core = me // 2, me % 2
    found = []
    for step in FAR_FIRST:
        there = lax.rem(chip + step + RING, RING)
        found += [2 * there + core, 2 * there + 1 - core]
    return found + [2 * chip + 1 - core]


def block(i):
    return pl.ds(pl.multiple_of(i * LANES, LANES), LANES)


def wait_for(ref, sem):
    pltpu.make_async_copy(ref, ref, sem).wait()


def exchange(
    w_gate, avg_gate, w_up, avg_up, w_down, avg_down, router_weight, router_gain,
    out, own_total, router,
    fresh, change, raw, raw_change, weight, gain,
    even, odd, parts, got, total, totals, late_parts, late_got, late_total, late_totals, inverse, ready, rows, columns,
    load_sem, part_send, part_recv, total_send, total_recv,
    late_part_send, late_part_recv, late_total_send, late_total_recv,
    send, recv, row_send, row_recv, column_send, column_recv,
):
    me, group = lax.axis_index("fsdp"), lax.axis_index("ep")
    barrier = pltpu.get_barrier_semaphore()

    peers = others(me)

    def greet(where):
        pl.semaphore_signal(barrier, inc=1, device_id=where, device_id_type=MESH)

    for d in peers:
        greet({"fsdp": d})
    loads = []
    for w, avg, at in ((w_gate, avg_gate, 0), (w_up, avg_up, EACH)):
        for e in range(EACH):
            loads.append((w.at[e], fresh.at[at + e]))
            loads.append((avg.at[e], change.at[at + e]))
    for e in range(EACH):
        loads.append((w_down.at[e], raw.at[e]))
        loads.append((avg_down.at[e], raw_change.at[e]))
    loads += [(router_weight, weight), (router_gain, gain)]
    loads = [pltpu.make_async_copy(a, b, load_sem.at[i]) for i, (a, b) in enumerate(loads)]
    for copy in loads[-2:] + [loads[2 * u + i] for u in IN_ORDER for i in range(2)]:
        copy.start()
    for i in range(1, PEERS):
        greet({"ep": lax.rem(group + i, PEERS)})

    def push(src, dst, send_sem, recv_sem, where, priority=0):
        pltpu.make_async_remote_copy(
            src_ref=src, dst_ref=dst, send_sem=send_sem, recv_sem=recv_sem, device_id=where, device_id_type=MESH
        ).start(priority=priority)

    low = lax.broadcasted_iota(jnp.int32, (SOON, LANES), 1) < HALF

    def split(rows, to):
        for z in range(RING):
            a, b = even[rows, LANES * z : LANES * (z + 1)], odd[rows, LANES * z : LANES * (z + 1)]
            to[2 * z, 0:SOON, :] = jnp.where(low, a, pltpu.roll(b, HALF, 1))
            to[2 * z + 1, 0:SOON, :] = jnp.where(low, pltpu.roll(a, HALF, 1), b)

    for done, u in enumerate(IN_ORDER):
        if done == 1:
            loads[-2].wait()
            loads[-1].wait()
            rows[:, block(me)] = (weight[...] * gain[...]).astype(jnp.bfloat16)
        if done == 2 * SOON:
            split(slice(0, SOON), parts)
            first = jnp.concatenate([even[0:1, LANES * z : LANES * (z + 1)] for z in range(RING)], axis=0)
            for d in range(PEERS):
                parts[d, SOON : SOON + RING, :] = first
            got[me] = parts[me]
        if done == BEFORE_BARRIER:
            pl.semaphore_wait(barrier, 2 * (PEERS - 1))
            for d in peers:
                push(parts.at[d], got.at[me], part_send, part_recv, {"fsdp": d})
        loads[2 * u].wait()
        loads[2 * u + 1].wait()
        sums, row = (even, odd)[u % 2], u // 2
        if u < 2 * EACH:

            def add_up(i, acc):
                at = pl.ds(pl.multiple_of(i * 16, 16), 16)
                x = fresh[u, at, :] + change[u, at, :].astype(jnp.float32)
                fresh[u, at, :] = x
                x = x * x
                return acc + x[:8] + x[8:]

            acc = lax.fori_loop(0, 8, add_up, jnp.zeros((8, 1024), jnp.float32), unroll=True)
            sums[row : row + 1, :] = jnp.sum(acc, axis=0, keepdims=True)
        else:
            e = u - 2 * EACH

            def add_across(b, _):
                x = raw[e, block(b), :] + raw_change[e, block(b), :].astype(jnp.float32)
                x = x.T
                fresh[u, :, block(b)] = x
                sums[row : row + 1, block(b)] = jnp.sum(x * x, axis=0, keepdims=True)
                return 0

            lax.fori_loop(0, 8, add_across, 0, unroll=True)
    split(slice(SOON, PAIRS), late_parts)
    late_got[me] = late_parts[me]
    for d in peers:
        push(late_parts.at[d], late_got.at[me], late_part_send, late_part_recv, {"fsdp": d})
    for d in peers:
        push(rows.at[:, block(me)], rows.at[:, block(me)], row_send, row_recv, {"fsdp": d})

    def normalise(u):
        for z in range(RING):
            x = fresh[u, :, LANES * z : LANES * (z + 1)] * inverse[u, z : z + 1, :]
            x = x.T.astype(jnp.bfloat16)
            ready[u, 2 * z] = x[:HALF]
            ready[u, 2 * z + 1] = x[HALF:]
        out[u, :, block(me)] = ready[u, me]

    def to_peer(u, d):
        push(ready.at[u, d], out.at[u, :, block(me)], send.at[u], recv.at[u], {"fsdp": d})

    def spread(u):
        for d in peers:
            to_peer(u, d)

    def sum_of(each):
        summed = each[0]
        for d in range(1, PEERS):
            summed = summed + each[d]
        return summed

    def invert(each, row):
        for z in range(RING):
            a, b = 1.0 / jnp.sqrt(each[2 * z]), 1.0 / jnp.sqrt(each[2 * z + 1])
            c, d = jnp.where(low, a, pltpu.roll(b, HALF, 1)), jnp.where(low, pltpu.roll(a, HALF, 1), b)
            for r in range(SOON):
                inverse[2 * (row + r), z : z + 1, :] = c[r : r + 1]
                inverse[2 * (row + r) + 1, z : z + 1, :] = d[r : r + 1]

    wait_for(got.at[pl.ds(0, PEERS - 1)], part_recv)
    summed = sum_of(got)
    total[...] = summed[:SOON]
    totals[me] = summed[:SOON]
    own_total[0:SOON, :] = summed[:SOON]
    inverse[0] = 1.0 / jnp.sqrt(summed[SOON:])
    for d in peers:
        push(total, totals.at[me], total_send, total_recv, {"fsdp": d})
    normalise(0)
    spread(0)

    wait_for(late_got.at[pl.ds(0, PEERS - 1)], late_part_recv)
    late_total[...] = sum_of(late_got)
    late_totals[me] = late_total[...]
    own_total[SOON:PAIRS, :] = late_total[...]
    for d in peers:
        push(late_total, late_totals.at[me], late_total_send, late_total_recv, {"fsdp": d})

    wait_for(totals.at[pl.ds(0, PEERS - 1)], total_recv)
    invert(totals, 0)

    def step(u, _):
        normalise(u + 1)
        spread(u)
        return 0

    def lead(d):
        return sum((d < 2 * chips).astype(jnp.int32) for chips in AHEAD)

    def spread_ahead(u, opens):
        for d in peers:
            if opens:
                to_peer(u, d)
                for i in range(1, len(AHEAD) + 1):
                    pl.when(lead(d) >= i)(lambda d=d, i=i: to_peer(u + i, d))
            else:
                unit = u + lead(d)
                pl.when(unit < UNITS)(lambda unit=unit, d=d: to_peer(unit, d))

    def step_ahead(u, _):
        pl.when(u + len(AHEAD) < UNITS)(lambda: normalise(u + len(AHEAD)))
        spread_ahead(u, False)
        return 0

    normalise(1)
    lax.fori_loop(1, 2 * SOON - 1, step, 0)
    spread(2 * SOON - 1)
    wait_for(late_totals.at[pl.ds(0, PEERS - 1)], late_total_recv)
    invert(late_totals, SOON)
    normalise(2 * SOON)
    lax.fori_loop(2 * SOON, SHIFT, step, 0)
    for i in range(1, len(AHEAD) + 1):
        normalise(SHIFT + i)
    spread_ahead(SHIFT, True)
    lax.fori_loop(SHIFT + 1, UNITS, step_ahead, 0)

    wait_for(rows.at[:, pl.ds(0, LANES * (PEERS - 1))], row_recv)
    columns[group] = rows[...]

    def to_group(i, _):
        push(rows, columns.at[group], column_send, column_recv, {"ep": lax.rem(group + i, PEERS)})
        return 0

    lax.fori_loop(1, PEERS, to_group, 0)

    wait_for(columns.at[pl.ds(0, PEERS - 1)], column_recv)
    for p in range(PEERS):
        router[4 * p : 4 * p + 4, :] = columns[p]

    def arrive(u, _):
        wait_for(out.at[u, :, pl.ds(0, LANES * (PEERS - 1))], recv.at[u])
        wait_for(ready.at[u, pl.ds(0, PEERS - 1)], send.at[u])
        return 0

    lax.fori_loop(0, UNITS, arrive, 0)
    wait_for(parts.at[pl.ds(0, PEERS - 1)], part_send)
    wait_for(totals.at[pl.ds(0, PEERS - 1)], total_send)
    wait_for(late_parts.at[pl.ds(0, PEERS - 1)], late_part_send)
    wait_for(late_totals.at[pl.ds(0, PEERS - 1)], late_total_send)
    wait_for(rows.at[:, pl.ds(0, LANES * (PEERS - 1))], row_send)
    wait_for(columns.at[pl.ds(0, PEERS - 1)], column_send)


def settle(
    out, own_total, router, gate, up, down, scale_gate, scale_up, scale_down, serve_router, a, b, c, sem
):
    copies = [(out.at[pl.ds(EACH * i, EACH)], to) for i, to in enumerate((gate, up, down))]
    copies.append((router, serve_router))
    copies += [(a, scale_gate), (b, scale_up), (c, scale_down)]
    copies = [pltpu.make_async_copy(x, y, sem.at[i]) for i, (x, y) in enumerate(copies)]
    for copy in copies[:4]:
        copy.start()
    for i, scale in enumerate((a, b, c)):
        for e in range(EACH):
            r, h = divmod(EACH * i + e, 2)
            scale[e : e + 1, :] = jnp.sqrt(own_total[r : r + 1, HALF * h : HALF * (h + 1)])
    for copy in copies[4:]:
        copy.start()
    for copy in copies:
        copy.wait()


def on_device(w_gate, avg_gate, w_up, avg_up, w_down, avg_down, router_weight, router_gain):
    f32, bf16 = jnp.float32, jnp.bfloat16
    hbm, vmem = pl.BlockSpec(memory_space=pltpu.HBM), pl.BlockSpec(memory_space=pltpu.VMEM)
    dma = pltpu.SemaphoreType.DMA
    held = pl.pallas_call(
        exchange,
        out_shape=(
            pltpu.VMEM((UNITS, HALF, 2048), bf16),
            pltpu.VMEM((PAIRS, LANES), f32),
            pltpu.VMEM((HALF, 2048), bf16),
        ),
        in_specs=[hbm] * 8,
        out_specs=(vmem,) * 3,
        scratch_shapes=[
            pltpu.VMEM((UNITS, LANES, 1024), f32),
            pltpu.VMEM((2 * EACH, LANES, 1024), bf16),
            pltpu.VMEM((EACH, 1024, LANES), f32),
            pltpu.VMEM((EACH, 1024, LANES), bf16),
            pltpu.VMEM((4, LANES), f32),
            pltpu.VMEM((1, LANES), f32),
            pltpu.VMEM((8, 1024), f32),
            pltpu.VMEM((8, 1024), f32),
            pltpu.VMEM((PEERS, SOON + RING, LANES), f32),
            pltpu.VMEM((PEERS, SOON + RING, LANES), f32),
            pltpu.VMEM((SOON, LANES), f32),
            pltpu.VMEM((PEERS, SOON, LANES), f32),
            pltpu.VMEM((PEERS, PAIRS - SOON, LANES), f32),
            pltpu.VMEM((PEERS, PAIRS - SOON, LANES), f32),
            pltpu.VMEM((PAIRS - SOON, LANES), f32),
            pltpu.VMEM((PEERS, PAIRS - SOON, LANES), f32),
            pltpu.VMEM((UNITS, RING, LANES), f32),
            pltpu.VMEM((UNITS, PEERS, HALF, LANES), bf16),
            pltpu.VMEM((4, 2048), bf16),
            pltpu.VMEM((PEERS, 4, 2048), bf16),
            dma((2 * UNITS + 2,)),
            dma(()), dma(()), dma(()), dma(()), dma(()), dma(()), dma(()), dma(()),
            dma((UNITS,)), dma((UNITS,)),
            dma(()), dma(()), dma(()), dma(()),
        ],
        compiler_params=pltpu.CompilerParams(
            collective_id=0, has_side_effects=True, vmem_limit_bytes=60 << 20
        ),
        name="exchange",
    )(w_gate, avg_gate, w_up, avg_up, w_down, avg_down, router_weight.T, router_gain[None, :])
    served = jax.ShapeDtypeStruct((EACH, HALF, 2048), bf16)
    scale = jax.ShapeDtypeStruct((EACH, HALF), f32)
    gate, up, down, scale_gate, scale_up, scale_down, router = pl.pallas_call(
        settle,
        out_shape=(served, served, served, scale, scale, scale, jax.ShapeDtypeStruct((HALF, 2048), bf16)),
        in_specs=[vmem] * 3,
        out_specs=(hbm,) * 7,
        scratch_shapes=[pltpu.VMEM((EACH, HALF), f32)] * 3 + [dma((7,))],
        compiler_params=pltpu.CompilerParams(vmem_limit_bytes=8 << 20),
        name="settle",
    )(*held)
    turned = (0, 2, 1)
    return (
        gate.transpose(turned), up.transpose(turned), down, scale_gate, scale_up, scale_down, router.T
    )


def solution(mesh):
    placed = (
        P("ep", "fsdp", None),
        P("ep", "fsdp", None),
        P("ep", "fsdp", None),
        P("ep", "fsdp", None),
        P("ep", None, "fsdp"),
        P("ep", None, "fsdp"),
        P("fsdp", "ep"),
        P("fsdp"),
    )
    return jax.shard_map(
        on_device,
        mesh=mesh,
        in_specs=placed,
        out_specs=(
            P("ep", None, "fsdp"),
            P("ep", None, "fsdp"),
            P("ep", "fsdp", None),
            P("ep", "fsdp"),
            P("ep", "fsdp"),
            P("ep", "fsdp"),
            P(),
        ),
        check_vma=False,
    )
```

```python
import jax
import jax.numpy as jnp
from jax import lax
from jax.experimental import pallas as pl
from jax.experimental.pallas import tpu as pltpu
from jax.sharding import PartitionSpec as P

MESH = pl.DeviceIdType.MESH
RING = 8
PEERS = 2 * RING
WIDE = (2, -2)
AHEAD = (2, 1)
SHIFT = 8
EACH = 4
UNITS = 3 * EACH
LANES = 128
HALF = 64
PAIRS = UNITS // 2
SOON = 3
LAST = UNITS - 1
IN_ORDER = tuple(range(2 * SOON)) + tuple(range(2 * EACH, UNITS)) + tuple(range(2 * SOON, 2 * EACH))
BEFORE_BARRIER = 10
FAR_FIRST = (4, 3, -3, 2, -2, 1, -1)


def others(me):
    chip, core = me // 2, me % 2
    found = []
    for step in FAR_FIRST:
        there = lax.rem(chip + step + RING, RING)
        found += [2 * there + core, 2 * there + 1 - core]
    return found + [2 * chip + 1 - core]


def block(i):
    return pl.ds(pl.multiple_of(i * LANES, LANES), LANES)


def wait_for(ref, sem):
    pltpu.make_async_copy(ref, ref, sem).wait()


def exchange(
    w_gate, avg_gate, w_up, avg_up, w_down, avg_down, router_weight, router_gain,
    out, own_total, router,
    fresh, change, raw, raw_change, weight, gain,
    even, odd, wide, widened, parts, got, total, totals, late_parts, late_got, late_total, late_totals, inverse, ready, rows, columns,
    load_sem, part_send, part_recv, total_send, total_recv,
    late_part_send, late_part_recv, late_total_send, late_total_recv,
    send, recv, wide_send, wide_recv, row_send, row_recv, column_send, column_recv,
):
    me, group = lax.axis_index("fsdp"), lax.axis_index("ep")
    barrier = pltpu.get_barrier_semaphore()

    peers = others(me)
    chip, core = me // 2, me % 2

    def greet(where):
        pl.semaphore_signal(barrier, inc=1, device_id=where, device_id_type=MESH)

    for d in peers:
        greet({"fsdp": d})
    loads = []
    for w, avg, at in ((w_gate, avg_gate, 0), (w_up, avg_up, EACH)):
        for e in range(EACH):
            loads.append((w.at[e], fresh.at[at + e]))
            loads.append((avg.at[e], change.at[at + e]))
    for e in range(EACH):
        loads.append((w_down.at[e], raw.at[e]))
        loads.append((avg_down.at[e], raw_change.at[e]))
    loads += [(router_weight, weight), (router_gain, gain)]
    loads = [pltpu.make_async_copy(a, b, load_sem.at[i]) for i, (a, b) in enumerate(loads)]
    for copy in loads[-2:] + [loads[2 * u + i] for u in IN_ORDER for i in range(2)]:
        copy.start()
    for i in range(1, PEERS):
        greet({"ep": lax.rem(group + i, PEERS)})

    def push(src, dst, send_sem, recv_sem, where, priority=0):
        pltpu.make_async_remote_copy(
            src_ref=src, dst_ref=dst, send_sem=send_sem, recv_sem=recv_sem, device_id=where, device_id_type=MESH
        ).start(priority=priority)

    low = lax.broadcasted_iota(jnp.int32, (SOON, LANES), 1) < HALF

    def split(rows, to):
        for z in range(RING):
            a, b = even[rows, LANES * z : LANES * (z + 1)], odd[rows, LANES * z : LANES * (z + 1)]
            to[2 * z, 0:SOON, :] = jnp.where(low, a, pltpu.roll(b, HALF, 1))
            to[2 * z + 1, 0:SOON, :] = jnp.where(low, pltpu.roll(a, HALF, 1), b)

    for done, u in enumerate(IN_ORDER):
        if done == 1:
            loads[-2].wait()
            loads[-1].wait()
            rows[:, block(me)] = (weight[...] * gain[...]).astype(jnp.bfloat16)
        if done == 2 * SOON:
            split(slice(0, SOON), parts)
            first = jnp.concatenate([even[0:1, LANES * z : LANES * (z + 1)] for z in range(RING)], axis=0)
            for d in range(PEERS):
                parts[d, SOON : SOON + RING, :] = first
            got[me] = parts[me]
        if done == BEFORE_BARRIER:
            for i, step in enumerate(WIDE):
                x = fresh[LAST, :, block(lax.rem(chip + step + RING, RING))].T
                wide[2 * i] = x[:HALF]
                wide[2 * i + 1] = x[HALF:]
            pl.semaphore_wait(barrier, 2 * (PEERS - 1))
            for d in peers:
                push(parts.at[d], got.at[me], part_send, part_recv, {"fsdp": d})
        loads[2 * u].wait()
        loads[2 * u + 1].wait()
        sums, row = (even, odd)[u % 2], u // 2
        if u < 2 * EACH:

            def add_up(i, acc):
                at = pl.ds(pl.multiple_of(i * 16, 16), 16)
                x = fresh[u, at, :] + change[u, at, :].astype(jnp.float32)
                fresh[u, at, :] = x
                x = x * x
                return acc + x[:8] + x[8:]

            acc = lax.fori_loop(0, 8, add_up, jnp.zeros((8, 1024), jnp.float32), unroll=True)
            sums[row : row + 1, :] = jnp.sum(acc, axis=0, keepdims=True)
        else:
            e = u - 2 * EACH

            def add_across(b, _):
                x = raw[e, block(b), :] + raw_change[e, block(b), :].astype(jnp.float32)
                x = x.T
                fresh[u, :, block(b)] = x
                sums[row : row + 1, block(b)] = jnp.sum(x * x, axis=0, keepdims=True)
                return 0

            lax.fori_loop(0, 8, add_across, 0, unroll=True)
    split(slice(SOON, PAIRS), late_parts)
    late_got[me] = late_parts[me]
    for d in peers:
        push(late_parts.at[d], late_got.at[me], late_part_send, late_part_recv, {"fsdp": d})
    for i, step in enumerate(WIDE):
        for c in range(2):
            there = 2 * lax.rem(chip + step + RING, RING) + c
            push(wide.at[2 * i + c], widened.at[2 * i + core], wide_send, wide_recv, {"fsdp": there})
    for d in peers:
        push(rows.at[:, block(me)], rows.at[:, block(me)], row_send, row_recv, {"fsdp": d})

    def normalise(u):
        for z in range(RING):
            x = fresh[u, :, LANES * z : LANES * (z + 1)] * inverse[u, z : z + 1, :]
            x = x.T.astype(jnp.bfloat16)
            ready[u, 2 * z] = x[:HALF]
            ready[u, 2 * z + 1] = x[HALF:]
        out[u, :, block(me)] = ready[u, me]

    def to_peer(u, d):
        push(ready.at[u, d], out.at[u, :, block(me)], send.at[u], recv.at[u], {"fsdp": d})

    def spread(u):
        for d in peers:
            to_peer(u, d)

    def sum_of(each):
        summed = each[0]
        for d in range(1, PEERS):
            summed = summed + each[d]
        return summed

    def invert(each, row):
        for z in range(RING):
            a, b = 1.0 / jnp.sqrt(each[2 * z]), 1.0 / jnp.sqrt(each[2 * z + 1])
            c, d = jnp.where(low, a, pltpu.roll(b, HALF, 1)), jnp.where(low, pltpu.roll(a, HALF, 1), b)
            for r in range(SOON):
                inverse[2 * (row + r), z : z + 1, :] = c[r : r + 1]
                inverse[2 * (row + r) + 1, z : z + 1, :] = d[r : r + 1]

    wait_for(got.at[pl.ds(0, PEERS - 1)], part_recv)
    summed = sum_of(got)
    total[...] = summed[:SOON]
    totals[me] = summed[:SOON]
    own_total[0:SOON, :] = summed[:SOON]
    inverse[0] = 1.0 / jnp.sqrt(summed[SOON:])
    for d in peers:
        push(total, totals.at[me], total_send, total_recv, {"fsdp": d})
    normalise(0)
    spread(0)

    wait_for(late_got.at[pl.ds(0, PEERS - 1)], late_part_recv)
    late_total[...] = sum_of(late_got)
    late_totals[me] = late_total[...]
    own_total[SOON:PAIRS, :] = late_total[...]
    for d in peers:
        push(late_total, late_totals.at[me], late_total_send, late_total_recv, {"fsdp": d})

    wait_for(totals.at[pl.ds(0, PEERS - 1)], total_recv)
    invert(totals, 0)

    def step(u, _):
        normalise(u + 1)
        spread(u)
        return 0

    def lead(d):
        return sum((d < 2 * chips).astype(jnp.int32) for chips in AHEAD)

    def spread_ahead(u, opens):
        for i, d in enumerate(peers):
            end = LAST if i < 2 * RING - 2 and FAR_FIRST[i // 2] in WIDE else UNITS
            if opens:
                to_peer(u, d)
                for i in range(1, len(AHEAD) + 1):
                    pl.when(lead(d) >= i)(lambda d=d, i=i: to_peer(u + i, d))
            else:
                unit = u + lead(d)
                pl.when(unit < end)(lambda unit=unit, d=d: to_peer(unit, d))

    def step_ahead(u, _):
        pl.when(u + len(AHEAD) < UNITS)(lambda: normalise(u + len(AHEAD)))
        spread_ahead(u, False)
        return 0

    normalise(1)
    lax.fori_loop(1, 2 * SOON - 1, step, 0)
    spread(2 * SOON - 1)
    wait_for(late_totals.at[pl.ds(0, PEERS - 1)], late_total_recv)
    invert(late_totals, SOON)
    normalise(2 * SOON)
    lax.fori_loop(2 * SOON, SHIFT, step, 0)
    for i in range(1, len(AHEAD) + 1):
        normalise(SHIFT + i)
    spread_ahead(SHIFT, True)
    lax.fori_loop(SHIFT + 1, UNITS, step_ahead, 0)

    wait_for(rows.at[:, pl.ds(0, LANES * (PEERS - 1))], row_recv)
    columns[group] = rows[...]

    def to_group(i, _):
        push(rows, columns.at[group], column_send, column_recv, {"ep": lax.rem(group + i, PEERS)})
        return 0

    lax.fori_loop(1, PEERS, to_group, 0)

    wait_for(columns.at[pl.ds(0, PEERS - 1)], column_recv)
    for p in range(PEERS):
        router[4 * p : 4 * p + 4, :] = columns[p]

    def arrive(u, _):
        wait_for(out.at[u, :, pl.ds(0, LANES * (PEERS - 1))], recv.at[u])
        wait_for(ready.at[u, pl.ds(0, PEERS - 1)], send.at[u])
        return 0

    by_row = jnp.broadcast_to(1.0 / jnp.sqrt(own_total[LAST // 2 : LAST // 2 + 1, :]), (LANES, LANES)).T
    by_row = by_row[HALF * (LAST % 2) : HALF * (LAST % 2 + 1)]
    wait_for(widened, wide_recv)
    for i, step in enumerate(WIDE):
        there = lax.rem(chip - step + RING, RING)
        for c in range(2):
            out[LAST, :, block(2 * there + c)] = (widened[2 * i + c] * by_row).astype(jnp.bfloat16)

    lax.fori_loop(0, LAST, arrive, 0)
    narrow = PEERS - 1 - 2 * len(WIDE)
    wait_for(out.at[LAST, :, pl.ds(0, LANES * narrow)], recv.at[LAST])
    wait_for(ready.at[LAST, pl.ds(0, narrow)], send.at[LAST])
    wait_for(wide, wide_send)
    wait_for(parts.at[pl.ds(0, PEERS - 1)], part_send)
    wait_for(totals.at[pl.ds(0, PEERS - 1)], total_send)
    wait_for(late_parts.at[pl.ds(0, PEERS - 1)], late_part_send)
    wait_for(late_totals.at[pl.ds(0, PEERS - 1)], late_total_send)
    wait_for(rows.at[:, pl.ds(0, LANES * (PEERS - 1))], row_send)
    wait_for(columns.at[pl.ds(0, PEERS - 1)], column_send)


def settle(
    out, own_total, router, gate, up, down, scale_gate, scale_up, scale_down, serve_router, a, b, c, sem
):
    copies = [(out.at[pl.ds(EACH * i, EACH)], to) for i, to in enumerate((gate, up, down))]
    copies.append((router, serve_router))
    copies += [(a, scale_gate), (b, scale_up), (c, scale_down)]
    copies = [pltpu.make_async_copy(x, y, sem.at[i]) for i, (x, y) in enumerate(copies)]
    for copy in copies[:4]:
        copy.start()
    for i, scale in enumerate((a, b, c)):
        for e in range(EACH):
            r, h = divmod(EACH * i + e, 2)
            scale[e : e + 1, :] = jnp.sqrt(own_total[r : r + 1, HALF * h : HALF * (h + 1)])
    for copy in copies[4:]:
        copy.start()
    for copy in copies:
        copy.wait()


def on_device(w_gate, avg_gate, w_up, avg_up, w_down, avg_down, router_weight, router_gain):
    f32, bf16 = jnp.float32, jnp.bfloat16
    hbm, vmem = pl.BlockSpec(memory_space=pltpu.HBM), pl.BlockSpec(memory_space=pltpu.VMEM)
    dma = pltpu.SemaphoreType.DMA
    held = pl.pallas_call(
        exchange,
        out_shape=(
            pltpu.VMEM((UNITS, HALF, 2048), bf16),
            pltpu.VMEM((PAIRS, LANES), f32),
            pltpu.VMEM((HALF, 2048), bf16),
        ),
        in_specs=[hbm] * 8,
        out_specs=(vmem,) * 3,
        scratch_shapes=[
            pltpu.VMEM((UNITS, LANES, 1024), f32),
            pltpu.VMEM((2 * EACH, LANES, 1024), bf16),
            pltpu.VMEM((EACH, 1024, LANES), f32),
            pltpu.VMEM((EACH, 1024, LANES), bf16),
            pltpu.VMEM((4, LANES), f32),
            pltpu.VMEM((1, LANES), f32),
            pltpu.VMEM((8, 1024), f32),
            pltpu.VMEM((8, 1024), f32),
            pltpu.VMEM((2 * len(WIDE), HALF, LANES), f32),
            pltpu.VMEM((2 * len(WIDE), HALF, LANES), f32),
            pltpu.VMEM((PEERS, SOON + RING, LANES), f32),
            pltpu.VMEM((PEERS, SOON + RING, LANES), f32),
            pltpu.VMEM((SOON, LANES), f32),
            pltpu.VMEM((PEERS, SOON, LANES), f32),
            pltpu.VMEM((PEERS, PAIRS - SOON, LANES), f32),
            pltpu.VMEM((PEERS, PAIRS - SOON, LANES), f32),
            pltpu.VMEM((PAIRS - SOON, LANES), f32),
            pltpu.VMEM((PEERS, PAIRS - SOON, LANES), f32),
            pltpu.VMEM((UNITS, RING, LANES), f32),
            pltpu.VMEM((UNITS, PEERS, HALF, LANES), bf16),
            pltpu.VMEM((4, 2048), bf16),
            pltpu.VMEM((PEERS, 4, 2048), bf16),
            dma((2 * UNITS + 2,)),
            dma(()), dma(()), dma(()), dma(()), dma(()), dma(()), dma(()), dma(()),
            dma((UNITS,)), dma((UNITS,)), dma(()), dma(()),
            dma(()), dma(()), dma(()), dma(()),
        ],
        compiler_params=pltpu.CompilerParams(
            collective_id=0, has_side_effects=True, vmem_limit_bytes=60 << 20
        ),
        name="exchange",
    )(w_gate, avg_gate, w_up, avg_up, w_down, avg_down, router_weight.T, router_gain[None, :])
    served = jax.ShapeDtypeStruct((EACH, HALF, 2048), bf16)
    scale = jax.ShapeDtypeStruct((EACH, HALF), f32)
    gate, up, down, scale_gate, scale_up, scale_down, router = pl.pallas_call(
        settle,
        out_shape=(served, served, served, scale, scale, scale, jax.ShapeDtypeStruct((HALF, 2048), bf16)),
        in_specs=[vmem] * 3,
        out_specs=(hbm,) * 7,
        scratch_shapes=[pltpu.VMEM((EACH, HALF), f32)] * 3 + [dma((7,))],
        compiler_params=pltpu.CompilerParams(vmem_limit_bytes=8 << 20),
        name="settle",
    )(*held)
    turned = (0, 2, 1)
    return (
        gate.transpose(turned), up.transpose(turned), down, scale_gate, scale_up, scale_down, router.T
    )


def solution(mesh):
    placed = (
        P("ep", "fsdp", None),
        P("ep", "fsdp", None),
        P("ep", "fsdp", None),
        P("ep", "fsdp", None),
        P("ep", None, "fsdp"),
        P("ep", None, "fsdp"),
        P("fsdp", "ep"),
        P("fsdp"),
    )
    return jax.shard_map(
        on_device,
        mesh=mesh,
        in_specs=placed,
        out_specs=(
            P("ep", None, "fsdp"),
            P("ep", None, "fsdp"),
            P("ep", "fsdp", None),
            P("ep", "fsdp"),
            P("ep", "fsdp"),
            P("ep", "fsdp"),
            P(),
        ),
        check_vma=False,
    )
```
